8 devices in a mesh: data: 4 (over z, y, x), pipe: 2 (over core).
Axes of the slice: x: 2, y: 2, z: 1, core: 2. Of those that a mesh axis runs over, the one named last changes fastest.
Arguments:
- acts_in: bfloat16 [128, 64, 1280], P(('data', 'pipe'))
- cot_out: bfloat16 [128, 64, 1280], P(('data', 'pipe'))
- seq_lens: int32 [128], P(('data', 'pipe'))
- w_qkv: bfloat16 [2, 1280, 3840], P('pipe')
- w_out: bfloat16 [2, 20, 64, 1280], P('pipe')
- w_up: bfloat16 [2, 1280, 5120], P('pipe')
- w_down: bfloat16 [2, 5120, 1280], P('pipe')
- gain_attn: bfloat16 [2, 1280], P('pipe')
- gain_mlp: bfloat16 [2, 1280], P('pipe')
Outputs:
- output 1: bfloat16 [128, 64, 1280], P(('data', 'pipe'))
- output 2: float32 [2, 1280, 3840], P('pipe')
- output 3: float32 [2, 20, 64, 1280], P('pipe')
- output 4: float32 [2, 1280, 5120], P('pipe')
- output 5: float32 [2, 5120, 1280], P('pipe')
- output 6: float32 [2, 1280], P('pipe')
- output 7: float32 [2, 1280], P('pipe')
All inputs are finite; a program needn't handle non-finite values.
Results may differ from the reference program's by a relative error of at most 0.02.
Values are sent between devices in bfloat16 or wider.
A program may use at most 1 GiB of HBM per device.

```python
import jax
import jax.numpy as jnp
from jax import lax

D = 1280
HEADS = 20
HEAD = 64
SEQ = 64
MICRO = 16
LAYERS_STAGE = 1
DATA_DEVS = 4
PIPE_DEVS = 2

NUM_LAYERS = PIPE_DEVS * LAYERS_STAGE
NUM_SEQS = DATA_DEVS * PIPE_DEVS * MICRO
FFN_DIM = 4 * D
MIN_LEN = SEQ // 4
NORM_EPS = 1e-5


def draw_lengths(key):
    key_len, key_perm = jax.random.split(key)
    len_draw = jax.random.randint(key_len, (NUM_SEQS,), MIN_LEN, SEQ + 1)
    rank_perm = jax.random.permutation(key_perm, NUM_SEQS)
    return jnp.where(rank_perm == 0, SEQ, jnp.where(rank_perm == 1, MIN_LEN, len_draw)).astype(jnp.int32)


def setup_inputs(seed: int = 0) -> dict:
    key_list = jax.random.split(jax.random.key(seed), 9)
    depth_scale = (2.0 / NUM_LAYERS) ** 0.5

    def normal_draw(key_idx, shape, scale):
        return (jax.random.normal(key_list[key_idx], shape, jnp.float32) * scale).astype(jnp.bfloat16)

    def gain_draw(key_idx):
        noise = jax.random.uniform(key_list[key_idx], (NUM_LAYERS, D), jnp.float32, -1.0, 1.0)
        return (1.0 + 0.5 * noise).astype(jnp.bfloat16)

    return {
        'acts_in': normal_draw(0, (NUM_SEQS, SEQ, D), 1.0),
        'cot_out': normal_draw(1, (NUM_SEQS, SEQ, D), (NUM_SEQS * SEQ) ** -0.5),
        'seq_lens': draw_lengths(key_list[2]),
        'w_qkv': normal_draw(3, (NUM_LAYERS, D, 3 * D), D ** -0.5),
        'w_out': normal_draw(4, (NUM_LAYERS, HEADS, HEAD, D), D ** -0.5),
        'w_up': normal_draw(5, (NUM_LAYERS, D, FFN_DIM), D ** -0.5),
        'w_down': normal_draw(6, (NUM_LAYERS, FFN_DIM, D), FFN_DIM ** -0.5 * depth_scale),
        'gain_attn': gain_draw(7),
        'gain_mlp': gain_draw(8),
    }


def rms_norm(hidden, gain):
    hid_f32 = hidden.astype(jnp.float32)
    inv_rms = lax.rsqrt(jnp.mean(hid_f32 * hid_f32, axis=-1, keepdims=True) + NORM_EPS)
    return (hid_f32 * inv_rms * gain.astype(jnp.float32)).astype(jnp.bfloat16)


def attend(qkv_all, seq_len):
    heads_all = qkv_all.astype(jnp.float32).reshape(SEQ, 3, HEADS, HEAD)
    scores = jnp.einsum('qhe,khe->hqk', heads_all[:, 0], heads_all[:, 1]) * HEAD ** -0.5
    positions = jnp.arange(SEQ)
    visible = (positions[None, :] <= positions[:, None]) & (positions[None, :] < seq_len)
    scores = jnp.where(visible[None], scores, -1e30)
    attn_probs = jax.nn.softmax(scores, axis=-1).astype(jnp.bfloat16)
    context = jnp.einsum('hqk,khe->qhe', attn_probs.astype(jnp.float32), heads_all[:, 2])
    return context.astype(jnp.bfloat16).reshape(SEQ, D)


def layer_apply(hidden, layer_w, seq_len):
    w_qkv, w_out, w_up, w_down, gain_attn, gain_mlp = layer_w
    qkv_all = jnp.dot(rms_norm(hidden, gain_attn), w_qkv, preferred_element_type=jnp.float32).astype(jnp.bfloat16)
    context = attend(qkv_all, seq_len)
    attn_out = jnp.dot(context, w_out.reshape(D, D), preferred_element_type=jnp.float32)
    mid_hidden = (hidden.astype(jnp.float32) + attn_out).astype(jnp.bfloat16)
    pre_act = jnp.dot(rms_norm(mid_hidden, gain_mlp), w_up, preferred_element_type=jnp.float32)
    gelu_out = jax.nn.gelu(pre_act, approximate=False).astype(jnp.bfloat16)
    mlp_out = jnp.dot(gelu_out, w_down, preferred_element_type=jnp.float32)
    return (mid_hidden.astype(jnp.float32) + mlp_out).astype(jnp.bfloat16)


def forward_seq(weights, seq_in, seq_len):
    def body(hidden, layer_w):
        return layer_apply(hidden, layer_w, seq_len), None

    hidden, _ = lax.scan(jax.checkpoint(body), seq_in, weights)
    valid = jnp.arange(SEQ)[:, None] < seq_len
    return jnp.where(valid, hidden, jnp.zeros_like(hidden))


def reference(acts_in, cot_out, seq_lens, w_qkv, w_out, w_up, w_down, gain_attn, gain_mlp):
    weights = (w_qkv, w_out, w_up, w_down, gain_attn, gain_mlp)

    def seq_step(grad_acc, seq_item):
        seq_in, seq_cot, seq_len = seq_item
        seq_out, pullback = jax.vjp(lambda layer_ws: forward_seq(layer_ws, seq_in, seq_len), weights)
        grad_seq = pullback(seq_cot)[0]
        new_acc = tuple(acc_part + grad_part.astype(jnp.float32) for acc_part, grad_part in zip(grad_acc, grad_seq))
        return new_acc, seq_out

    grad_init = tuple(jnp.zeros(w_part.shape, jnp.float32) for w_part in weights)
    grad_total, acts_out = lax.scan(seq_step, grad_init, (acts_in, cot_out, seq_lens))
    return (acts_out, grad_total[0], grad_total[1], grad_total[2], grad_total[3], grad_total[4], grad_total[5])
```

```python
import functools
import jax
import jax.numpy as jnp
from jax import lax
from jax.experimental import pallas as pl
from jax.experimental.pallas import tpu as pltpu
from jax.sharding import PartitionSpec as P


NORM_EPS = 1e-5
BF = jnp.bfloat16
F32 = jnp.float32
SEQ = 64
HEAD = 64
CHUNK = 64
NN = (((1,), (0,)), ((), ()))
NT = (((1,), (1,)), ((), ()))
TN = (((0,), (0,)), ((), ()))


def dot(lhs, rhs, dims=NN):
    return lax.dot_general(lhs, rhs, dims, preferred_element_type=F32)


def norm_fwd(hid, gain):
    inv_rms = lax.rsqrt(jnp.mean(hid * hid, axis=-1, keepdims=True) + NORM_EPS)
    return (hid * inv_rms * gain).astype(BF)


def norm_bwd(d_normed, hid, gain):
    inv_rms = lax.rsqrt(jnp.mean(hid * hid, axis=-1, keepdims=True) + NORM_EPS)
    unit = hid * inv_rms
    d_unit = d_normed * gain
    d_hid = inv_rms * (d_unit - unit * jnp.mean(d_unit * unit, axis=-1, keepdims=True))
    return d_hid, jnp.sum(d_normed * unit, axis=0)


def half_erf(pre):
    return 0.5 + 0.5 * lax.erf(pre * 0.7071067811865476)


def gelu_grad(pre, cdf):
    return cdf + pre * (jnp.exp(-0.5 * pre * pre) * 0.3989422804014327)


def mlp_fwd_body(rows, x_ref, res_ref, up_ref, down_ref, out_ref, pre_ref, acc_ref):
    step = pl.program_id(0)
    tokens = x_ref.shape[0]

    @pl.when(step == 0)
    def _():
        acc_ref[...] = res_ref[...].astype(F32)

    for start in range(0, tokens, rows):
        sl = pl.ds(start, rows)
        pre = dot(x_ref[sl, :], up_ref[0])
        pre_ref[sl, :] = pre
        act = (pre * half_erf(pre)).astype(BF)
        acc_ref[sl, :] += dot(act, down_ref[0])

    @pl.when(step == pl.num_programs(0) - 1)
    def _():
        out_ref[...] = acc_ref[...].astype(BF)


def mlp_fwd(normed, res, w_up, w_down, layer, fb=512, rows=512):
    tokens, dim = normed.shape
    ffn = w_up.shape[2]
    return pl.pallas_call(
        functools.partial(mlp_fwd_body, rows),
        grid=(ffn // fb,),
        in_specs=[
            pl.BlockSpec((tokens, dim), lambda f: (0, 0)),
            pl.BlockSpec((tokens, dim), lambda f: (0, 0)),
            pl.BlockSpec((1, dim, fb), lambda f: (layer, 0, f)),
            pl.BlockSpec((1, fb, dim), lambda f: (layer, f, 0)),
        ],
        out_specs=[
            pl.BlockSpec((tokens, dim), lambda f: (0, 0)),
            pl.BlockSpec((tokens, fb), lambda f: (0, f)),
        ],
        out_shape=[jax.ShapeDtypeStruct((tokens, dim), BF), jax.ShapeDtypeStruct((tokens, ffn), F32)],
        scratch_shapes=[pltpu.VMEM((tokens, dim), F32)],
        compiler_params=pltpu.CompilerParams(vmem_limit_bytes=56 * 1024 * 1024),
        cost_estimate=pl.CostEstimate(flops=4 * tokens * dim * ffn, bytes_accessed=4 * dim * ffn + 4 * tokens * ffn, transcendentals=tokens * ffn),
        name='mlp_fwd',
    )(normed, res, w_up, w_down)


def mlp_bwd_body(rows, dt_ref, pre_ref, up_ref, down_ref, out_ref):
    step = pl.program_id(0)
    tokens = dt_ref.shape[0]

    @pl.when(step == 0)
    def _():
        out_ref[...] = jnp.zeros_like(out_ref)

    for start in range(0, tokens, rows):
        sl = pl.ds(start, rows)
        d_act = dot(dt_ref[sl, :], down_ref[0], NT)
        pre = pre_ref[sl, :]
        d_pre = (d_act * gelu_grad(pre, half_erf(pre))).astype(BF)
        out_ref[sl, :] += dot(d_pre, up_ref[0], NT)


def mlp_bwd(d_top, pre, w_up, w_down, layer, fb=512, rows=512):
    tokens, dim = d_top.shape
    ffn = w_up.shape[2]
    return pl.pallas_call(
        functools.partial(mlp_bwd_body, rows),
        grid=(ffn // fb,),
        in_specs=[
            pl.BlockSpec((tokens, dim), lambda f: (0, 0)),
            pl.BlockSpec((tokens, fb), lambda f: (0, f)),
            pl.BlockSpec((1, dim, fb), lambda f: (layer, 0, f)),
            pl.BlockSpec((1, fb, dim), lambda f: (layer, f, 0)),
        ],
        out_specs=pl.BlockSpec((tokens, dim), lambda f: (0, 0)),
        out_shape=jax.ShapeDtypeStruct((tokens, dim), F32),
        compiler_params=pltpu.CompilerParams(vmem_limit_bytes=56 * 1024 * 1024),
        cost_estimate=pl.CostEstimate(flops=4 * tokens * dim * ffn, bytes_accessed=4 * dim * ffn + 4 * tokens * ffn, transcendentals=tokens * ffn),
        name='mlp_bwd',
    )(d_top, pre, w_up, w_down)


PER_TILE = 8
CHIPS = 4


def chunk_table_body(per_dev, count_ref, chip_ref, first_ref, tbl_ref):
    half = CHIPS * per_dev
    for group in range(2):
        def place(i, used, group=group):
            src, k = i // per_dev, i % per_dev
            live = k * CHUNK < count_ref[(src ^ chip_ref[0]) * 2 + group]
            slot = jnp.where(live, used, half - 1 - (i - used))
            tbl_ref[group * half + slot] = (src * 2 + group) * per_dev + k
            return used + jnp.where(live, 1, 0)

        used = lax.fori_loop(0, half, place, 0)
        tbl_ref[2 * half + group] = (used + PER_TILE - 1) // PER_TILE
    tbl_ref[2 * half + 2] = first_ref[0]


def chunk_table(counts, chip, first, per_dev):
    smem = pl.BlockSpec(memory_space=pltpu.SMEM)
    return pl.pallas_call(
        functools.partial(chunk_table_body, per_dev),
        in_specs=[smem] * 3,
        out_specs=smem,
        out_shape=jax.ShapeDtypeStruct((2 * CHIPS * per_dev + 3,), jnp.int32),
        name='chunk_table',
    )(counts, chip, first)


def mlp_grad_body(sub, half, tbl_ref, *refs):
    nm_refs, low_refs, high_refs, far_refs = (refs[k * PER_TILE:(k + 1) * PER_TILE] for k in range(4))
    up_ref, down_ref, gup_ref, gdown_ref, nm_s, dt_s = refs[4 * PER_TILE:]
    tile = pl.program_id(1)
    fb = up_ref.shape[1]
    near = tbl_ref[2 * half]
    low = tbl_ref[2 * half + 2] == 1

    @pl.when(tile == 0)
    def _():
        gup_ref[...] = jnp.zeros_like(gup_ref)
        gdown_ref[...] = jnp.zeros_like(gdown_ref)

    def take(dst, srcs):
        for k in range(PER_TILE):
            dst[pl.ds(k * CHUNK, CHUNK), :] = srcs[k][...]

    @pl.when(tile < near + tbl_ref[2 * half + 1])
    def _():
        take(nm_s, nm_refs)

        @pl.when((tile < near) & low)
        def _():
            take(dt_s, low_refs)

        @pl.when((tile < near) & jnp.logical_not(low))
        def _():
            take(dt_s, high_refs)

        @pl.when(tile >= near)
        def _():
            take(dt_s, far_refs)

        for start in range(0, fb, sub):
            sl = pl.ds(start, sub)
            pre = dot(nm_s[...], up_ref[:, sl])
            d_act = dot(dt_s[...], down_ref[sl, :], NT)
            cdf = half_erf(pre)
            act = (pre * cdf).astype(BF)
            gdown_ref[sl, :] += dot(act, dt_s[...], TN)
            d_pre = (d_act * gelu_grad(pre, cdf)).astype(BF)
            gup_ref[:, sl] += dot(nm_s[...], d_pre, TN)


def mlp_grad(table, normed_all, near_low, near_high, far, w_up, w_down, fb=1024, sub=512):
    tokens, dim = normed_all.shape
    ffn = w_up.shape[1]
    half = tokens // CHUNK // 2
    per_dev = half // CHIPS
    tiles = tokens // (CHUNK * PER_TILE)

    def group_chunk(entry):
        return entry // (2 * per_dev) * per_dev + entry % per_dev

    def any_spec(k):
        def index(f, t, tbl):
            near = tbl[2 * half]
            offset = jnp.where(t < near, t * PER_TILE, half + (jnp.minimum(t, near + tbl[2 * half + 1] - 1) - near) * PER_TILE)
            return tbl[offset + k], 0

        return pl.BlockSpec((CHUNK, dim), index)

    def near_spec(k, flag):
        def index(f, t, tbl):
            entry = group_chunk(tbl[jnp.minimum(t, tbl[2 * half] - 1) * PER_TILE + k])
            return jnp.where(tbl[2 * half + 2] == flag, entry, 0), 0

        return pl.BlockSpec((CHUNK, dim), index)

    def far_spec(k):
        def index(f, t, tbl):
            step = jnp.clip(t - tbl[2 * half], 0, tbl[2 * half + 1] - 1)
            return group_chunk(tbl[half + step * PER_TILE + k]), 0

        return pl.BlockSpec((CHUNK, dim), index)

    ks = range(PER_TILE)
    grid_spec = pltpu.PrefetchScalarGridSpec(
        num_scalar_prefetch=1,
        grid=(ffn // fb, tiles),
        in_specs=[any_spec(k) for k in ks] + [near_spec(k, 1) for k in ks] + [near_spec(k, 0) for k in ks] + [far_spec(k) for k in ks] + [
            pl.BlockSpec((dim, fb), lambda f, t, tbl: (0, f)),
            pl.BlockSpec((fb, dim), lambda f, t, tbl: (f, 0)),
        ],
        out_specs=[
            pl.BlockSpec((dim, fb), lambda f, t, tbl: (0, f)),
            pl.BlockSpec((fb, dim), lambda f, t, tbl: (f, 0)),
        ],
        scratch_shapes=[pltpu.VMEM((CHUNK * PER_TILE, dim), BF), pltpu.VMEM((CHUNK * PER_TILE, dim), BF)],
    )
    operands = [arr for arr in (normed_all, near_low, near_high, far) for _ in ks]
    return pl.pallas_call(
        functools.partial(mlp_grad_body, sub, half),
        grid_spec=grid_spec,
        out_shape=[jax.ShapeDtypeStruct((dim, ffn), F32), jax.ShapeDtypeStruct((ffn, dim), F32)],
        compiler_params=pltpu.CompilerParams(vmem_limit_bytes=62 * 1024 * 1024),
        cost_estimate=pl.CostEstimate(flops=8 * tokens * dim * ffn, bytes_accessed=12 * dim * ffn + 20 * tokens * dim, transcendentals=2 * tokens * ffn),
        name='mlp_grad',
    )(table, *operands, w_up, w_down)


def pair_mask(len_lo, len_hi):
    row = lax.broadcasted_iota(jnp.int32, (2 * SEQ, 2 * SEQ), 0)
    col = lax.broadcasted_iota(jnp.int32, (2 * SEQ, 2 * SEQ), 1)
    limit = jnp.where(row < SEQ, len_lo, len_hi + SEQ)
    floor = jnp.where(row < SEQ, 0, SEQ)
    return (col <= row) & (col < limit) & (col >= floor)


def head_masks():
    lane = lax.broadcasted_iota(jnp.int32, (1, 2 * HEAD), 1)
    low = jnp.where(lane < HEAD, 1.0, 0.0)
    return low.astype(BF), (1.0 - low).astype(BF)


def pair_softmax(query, key, visible):
    scores = jnp.where(visible, dot(query, key, NT) * HEAD ** -0.5, -1e30)
    weights = jnp.exp(scores - jnp.max(scores, axis=-1, keepdims=True))
    return weights * (1.0 / jnp.sum(weights, axis=-1, keepdims=True))


def attn_fwd_body(dim, len_ref, qkv_ref, ctx_ref):
    step = pl.program_id(0)
    visible = pair_mask(len_ref[2 * step], len_ref[2 * step + 1])
    masks = head_masks()
    for start in range(0, dim, 2 * HEAD):
        query = qkv_ref[:, pl.ds(start, 2 * HEAD)]
        key = qkv_ref[:, pl.ds(dim + start, 2 * HEAD)]
        value = qkv_ref[:, pl.ds(2 * dim + start, 2 * HEAD)]
        total = None
        for mask in masks:
            probs = pair_softmax(query * mask, key, visible).astype(BF)
            part = dot(probs, value * mask)
            total = part if total is None else total + part
        ctx_ref[:, pl.ds(start, 2 * HEAD)] = total.astype(BF)


def attn_fwd(lens, qkv):
    tokens, dim = qkv.shape[0], qkv.shape[1] // 3
    grid_spec = pltpu.PrefetchScalarGridSpec(
        num_scalar_prefetch=1,
        grid=(tokens // (2 * SEQ),),
        in_specs=[pl.BlockSpec((2 * SEQ, 3 * dim), lambda s, lens: (s, 0))],
        out_specs=pl.BlockSpec((2 * SEQ, dim), lambda s, lens: (s, 0)),
    )
    return pl.pallas_call(
        functools.partial(attn_fwd_body, dim),
        grid_spec=grid_spec,
        out_shape=jax.ShapeDtypeStruct((tokens, dim), BF),
        cost_estimate=pl.CostEstimate(flops=16 * tokens * 128 * dim, bytes_accessed=8 * tokens * dim, transcendentals=tokens * 128 * 20),
        name='attn_fwd',
    )(lens, qkv)


def attn_bwd_body(dim, len_ref, qkv_ref, dctx_ref, dqkv_ref):
    step = pl.program_id(0)
    visible = pair_mask(len_ref[2 * step], len_ref[2 * step + 1])
    masks = head_masks()
    for start in range(0, dim, 2 * HEAD):
        query = qkv_ref[:, pl.ds(start, 2 * HEAD)]
        key = qkv_ref[:, pl.ds(dim + start, 2 * HEAD)]
        value = qkv_ref[:, pl.ds(2 * dim + start, 2 * HEAD)]
        d_ctx = dctx_ref[:, pl.ds(start, 2 * HEAD)]
        d_query = d_key = d_value = 0.0
        for mask in masks:
            query_m, d_ctx_m = query * mask, d_ctx * mask
            probs = pair_softmax(query_m, key, visible)
            d_probs = dot(d_ctx_m, value, NT)
            inner = jnp.sum(probs * d_probs, axis=-1, keepdims=True)
            d_scores = (probs * (d_probs - inner) * HEAD ** -0.5).astype(BF)
            d_value = d_value + dot(probs.astype(BF), d_ctx_m, TN)
            d_query = d_query + dot(d_scores, key * mask)
            d_key = d_key + dot(d_scores, query_m, TN)
        dqkv_ref[:, pl.ds(start, 2 * HEAD)] = d_query.astype(BF)
        dqkv_ref[:, pl.ds(dim + start, 2 * HEAD)] = d_key.astype(BF)
        dqkv_ref[:, pl.ds(2 * dim + start, 2 * HEAD)] = d_value.astype(BF)


def attn_bwd(lens, qkv, d_ctx):
    tokens, dim = d_ctx.shape
    grid_spec = pltpu.PrefetchScalarGridSpec(
        num_scalar_prefetch=1,
        grid=(tokens // (2 * SEQ),),
        in_specs=[
            pl.BlockSpec((2 * SEQ, 3 * dim), lambda s, lens: (s, 0)),
            pl.BlockSpec((2 * SEQ, dim), lambda s, lens: (s, 0)),
        ],
        out_specs=pl.BlockSpec((2 * SEQ, 3 * dim), lambda s, lens: (s, 0)),
    )
    return pl.pallas_call(
        functools.partial(attn_bwd_body, dim),
        grid_spec=grid_spec,
        out_shape=jax.ShapeDtypeStruct((tokens, 3 * dim), BF),
        cost_estimate=pl.CostEstimate(flops=40 * tokens * 128 * dim, bytes_accessed=14 * tokens * dim, transcendentals=tokens * 128 * 20),
        name='attn_bwd',
    )(lens, qkv, d_ctx)


def solution(mesh):
    row_spec = P(('data', 'pipe'))
    stage_spec = P('pipe')
    swap = [(0, 1), (1, 0)]

    def flip_data(arr, bit):
        return lax.ppermute(arr, 'data', [(src, src ^ bit) for src in range(mesh.shape['data'])])

    def device_pass(acts_in, cot_out, seq_lens, w_qkv, w_out, w_up, w_down, gain_attn, gain_mlp):
        pipe = lax.axis_index('pipe')
        chip = lax.axis_index('data')
        seqs, seq, dim = acts_in.shape
        tokens = seqs * seq
        first = pipe == 0

        def gather_pair(part):
            return lax.all_gather(part, 'pipe', axis=0, tiled=True)

        wq = gather_pair(w_qkv)
        wo = gather_pair(w_out.reshape(1, dim, dim))
        wu = gather_pair(w_up)
        wd = gather_pair(w_down)
        gains_own = jnp.stack([gain_attn, gain_mlp], axis=1)
        gains_other = lax.ppermute(gains_own, 'pipe', swap)
        gains = jnp.where(first, jnp.concatenate([gains_own, gains_other]), jnp.concatenate([gains_other, gains_own])).astype(F32)

        pos = jnp.arange(seq)
        valid = pos[None, :] < seq_lens[:, None]
        cot = jnp.where(valid[:, :, None], cot_out, jnp.zeros_like(cot_out)).reshape(tokens, dim)

        order = jnp.arange(seqs)
        first_rank = jnp.sum(jnp.where(order[None, :] < order[:, None], seq_lens[None, :], 0), axis=1)
        rank = jnp.where(valid, first_rank[:, None] + pos[None, :], -1).reshape(1, tokens)
        pick = (rank == jnp.arange(tokens)[:, None]).astype(BF)

        count = jnp.full((8, 128), jnp.sum(seq_lens), jnp.int32)
        pair_counts = jnp.stack([count, lax.ppermute(count, 'pipe', swap)])
        half_counts = jnp.stack([pair_counts, flip_data(pair_counts, 1)])
        counts = jnp.concatenate([half_counts, flip_data(half_counts, 2)])[:, :, 0, 0].reshape(-1)
        table = chunk_table(counts, chip.astype(jnp.int32)[None], first.astype(jnp.int32)[None], tokens // CHUNK)

        cot_packed = dot(pick, cot_out.reshape(tokens, dim)).astype(BF)
        cot_group = lax.all_gather(cot_packed, 'data').reshape(-1, dim)

        saved = []
        hid = acts_in.reshape(tokens, dim)
        for layer in range(2):
            hid_f = hid.astype(F32)
            normed_a = norm_fwd(hid_f, gains[layer, 0])
            qkv = dot(normed_a, wq[layer]).astype(BF)
            ctx = attn_fwd(seq_lens, qkv)
            mid = (hid_f + dot(ctx, wo[layer])).astype(BF)
            normed_m = norm_fwd(mid.astype(F32), gains[layer, 1])
            out, pre = mlp_fwd(normed_m, mid, wu, wd, layer)
            saved.append((hid, normed_a, qkv, ctx, mid, normed_m, pre))
            hid = out
        acts_out = jnp.where(valid[:, :, None], hid.reshape(acts_in.shape), jnp.zeros_like(acts_in))

        def home(lower, upper):
            recv = lax.ppermute(jnp.where(first, upper, lower), 'pipe', swap)
            return jnp.where(first, lower, upper), recv

        nm_own = dot(pick, jnp.where(first, saved[0][5], saved[1][5])).astype(BF)
        nm_send = dot(pick, jnp.where(first, saved[1][5], saved[0][5])).astype(BF)
        nm_pair = jnp.stack([nm_own, lax.ppermute(nm_send, 'pipe', swap)])
        normed_all = lax.all_gather(nm_pair, 'data').reshape(-1, dim)
        na_home = home(saved[0][1], saved[1][1])
        ctx_home = home(saved[0][3], saved[1][3])

        d_hid = cot.astype(F32)
        d_mids, d_qkvs, d_gains = [None, None], [None, None], [None, None]
        for layer in (1, 0):
            hid_in, normed_a, qkv, ctx, mid, normed_m, pre = saved[layer]
            d_top = d_hid.astype(BF)
            if layer == 0:
                d_packed = dot(pick, d_top).astype(BF)
                d_group = lax.all_gather(d_packed, 'data').reshape(-1, dim)
            d_normed_m = mlp_bwd(d_top, pre, wu, wd, layer)
            d_norm, gain_m = norm_bwd(d_normed_m, mid.astype(F32), gains[layer, 1])
            d_mid = d_hid + d_norm
            d_mids[layer] = d_mid.astype(BF)
            d_ctx = dot(d_mids[layer], wo[layer], NT).astype(BF)
            d_qkvs[layer] = attn_bwd(seq_lens, qkv, d_ctx)
            d_normed_a = dot(d_qkvs[layer], wq[layer], NT)
            d_norm, gain_a = norm_bwd(d_normed_a, hid_in.astype(F32), gains[layer, 0])
            d_hid = d_mid + d_norm
            d_gains[layer] = jnp.stack([gain_a, gain_m])

        mid_home = home(*d_mids)
        qkv_home = home(*d_qkvs)
        g_qkv = dot(na_home[0], qkv_home[0], TN) + dot(na_home[1], qkv_home[1], TN)
        g_out = dot(ctx_home[0], mid_home[0], TN) + dot(ctx_home[1], mid_home[1], TN)

        d_group, g_qkv, g_out = lax.optimization_barrier((d_group, g_qkv, g_out))
        g_qkv, g_out = lax.psum((g_qkv, g_out), 'data')

        d_recv = lax.ppermute(jnp.where(first, cot_group, d_group), 'pipe', swap)
        grad_up, grad_down = mlp_grad(table, normed_all, d_group, cot_group, d_recv, w_up[0], w_down[0])

        gain_own, gain_recv = home(*d_gains)
        g_gain = gain_own + gain_recv
        g_gain = g_gain + flip_data(g_gain, 1)
        g_gain = g_gain + flip_data(g_gain, 2)
        return (acts_out, g_qkv[None], g_out.reshape(w_out.shape), grad_up[None], grad_down[None], g_gain[:1], g_gain[1:])

    return jax.shard_map(device_pass, mesh=mesh, in_specs=(row_spec, row_spec, row_spec) + (stage_spec,) * 6, out_specs=(row_spec,) + (stage_spec,) * 6, check_vma=False)
```

```python
import functools
import jax
import jax.numpy as jnp
from jax import lax
from jax.experimental import pallas as pl
from jax.experimental.pallas import tpu as pltpu
from jax.sharding import PartitionSpec as P


NORM_EPS = 1e-5
BF = jnp.bfloat16
F32 = jnp.float32
SEQ = 64
HEAD = 64
CHUNK = 64
NN = (((1,), (0,)), ((), ()))
NT = (((1,), (1,)), ((), ()))
TN = (((0,), (0,)), ((), ()))


def dot(lhs, rhs, dims=NN):
    return lax.dot_general(lhs, rhs, dims, preferred_element_type=F32)


def norm_fwd(hid, gain):
    inv_rms = lax.rsqrt(jnp.mean(hid * hid, axis=-1, keepdims=True) + NORM_EPS)
    return (hid * inv_rms * gain).astype(BF)


def norm_bwd(d_normed, hid, gain):
    inv_rms = lax.rsqrt(jnp.mean(hid * hid, axis=-1, keepdims=True) + NORM_EPS)
    unit = hid * inv_rms
    d_unit = d_normed * gain
    d_hid = inv_rms * (d_unit - unit * jnp.mean(d_unit * unit, axis=-1, keepdims=True))
    return d_hid, jnp.sum(d_normed * unit, axis=0)


def half_erf(pre):
    return 0.5 + 0.5 * lax.erf(pre * 0.7071067811865476)


def gelu_grad(pre, cdf):
    return cdf + pre * (jnp.exp(-0.5 * pre * pre) * 0.3989422804014327)


def mlp_fwd_body(rows, own_ref, x_ref, res_ref, own_up_ref, own_down_ref, far_up_ref, far_down_ref, out_ref, pre_ref, acc_ref):
    step = pl.program_id(0)
    tokens = x_ref.shape[0]

    @pl.when(step == 0)
    def _():
        acc_ref[...] = res_ref[...].astype(F32)

    def run(up_ref, down_ref):
        for start in range(0, tokens, rows):
            sl = pl.ds(start, rows)
            pre = dot(x_ref[sl, :], up_ref[0])
            pre_ref[sl, :] = pre
            act = (pre * half_erf(pre)).astype(BF)
            acc_ref[sl, :] += dot(act, down_ref[0])

    @pl.when(own_ref[0] == 1)
    def _():
        run(own_up_ref, own_down_ref)

    @pl.when(own_ref[0] == 0)
    def _():
        run(far_up_ref, far_down_ref)

    @pl.when(step == pl.num_programs(0) - 1)
    def _():
        out_ref[...] = acc_ref[...].astype(BF)


def weight_specs(dim, fb):
    return [
        pl.BlockSpec((1, dim, fb), lambda f, own: (0, 0, f * own[0])),
        pl.BlockSpec((1, fb, dim), lambda f, own: (0, f * own[0], 0)),
        pl.BlockSpec((1, dim, fb), lambda f, own: (0, 0, f * (1 - own[0]))),
        pl.BlockSpec((1, fb, dim), lambda f, own: (0, f * (1 - own[0]), 0)),
    ]


def mlp_fwd(own, normed, res, weights, fb=512, rows=512):
    tokens, dim = normed.shape
    ffn = weights[0].shape[2]
    whole = pl.BlockSpec((tokens, dim), lambda f, own: (0, 0))
    return pl.pallas_call(
        functools.partial(mlp_fwd_body, rows),
        grid_spec=pltpu.PrefetchScalarGridSpec(
            num_scalar_prefetch=1,
            grid=(ffn // fb,),
            in_specs=[whole, whole] + weight_specs(dim, fb),
            out_specs=[whole, pl.BlockSpec((tokens, fb), lambda f, own: (0, f))],
            scratch_shapes=[pltpu.VMEM((tokens, dim), F32)],
        ),
        out_shape=[jax.ShapeDtypeStruct((tokens, dim), BF), jax.ShapeDtypeStruct((tokens, ffn), F32)],
        compiler_params=pltpu.CompilerParams(vmem_limit_bytes=56 * 1024 * 1024),
        cost_estimate=pl.CostEstimate(flops=4 * tokens * dim * ffn, bytes_accessed=4 * dim * ffn + 4 * tokens * ffn, transcendentals=tokens * ffn),
        name='mlp_fwd',
    )(own, normed, res, *weights)


def mlp_bwd_body(rows, own_ref, dt_ref, pre_ref, own_up_ref, own_down_ref, far_up_ref, far_down_ref, out_ref):
    step = pl.program_id(0)
    tokens = dt_ref.shape[0]

    @pl.when(step == 0)
    def _():
        out_ref[...] = jnp.zeros_like(out_ref)

    def run(up_ref, down_ref):
        for start in range(0, tokens, rows):
            sl = pl.ds(start, rows)
            d_act = dot(dt_ref[sl, :], down_ref[0], NT)
            pre = pre_ref[sl, :]
            d_pre = (d_act * gelu_grad(pre, half_erf(pre))).astype(BF)
            out_ref[sl, :] += dot(d_pre, up_ref[0], NT)

    @pl.when(own_ref[0] == 1)
    def _():
        run(own_up_ref, own_down_ref)

    @pl.when(own_ref[0] == 0)
    def _():
        run(far_up_ref, far_down_ref)


def mlp_bwd(own, d_top, pre, weights, fb=512, rows=512):
    tokens, dim = d_top.shape
    ffn = weights[0].shape[2]
    whole = pl.BlockSpec((tokens, dim), lambda f, own: (0, 0))
    return pl.pallas_call(
        functools.partial(mlp_bwd_body, rows),
        grid_spec=pltpu.PrefetchScalarGridSpec(
            num_scalar_prefetch=1,
            grid=(ffn // fb,),
            in_specs=[whole, pl.BlockSpec((tokens, fb), lambda f, own: (0, f))] + weight_specs(dim, fb),
            out_specs=whole,
        ),
        out_shape=jax.ShapeDtypeStruct((tokens, dim), F32),
        compiler_params=pltpu.CompilerParams(vmem_limit_bytes=56 * 1024 * 1024),
        cost_estimate=pl.CostEstimate(flops=4 * tokens * dim * ffn, bytes_accessed=4 * dim * ffn + 4 * tokens * ffn, transcendentals=tokens * ffn),
        name='mlp_bwd',
    )(own, d_top, pre, *weights)


PER_TILE = 8
CHIPS = 4


def chunk_table_body(per_dev, count_ref, chip_ref, first_ref, tbl_ref):
    half = CHIPS * per_dev
    for group in range(2):
        def place(i, used, group=group):
            src, k = i // per_dev, i % per_dev
            live = k * CHUNK < count_ref[(src ^ chip_ref[0]) * 2 + group]
            slot = jnp.where(live, used, half - 1 - (i - used))
            tbl_ref[group * half + slot] = (src * 2 + group) * per_dev + k
            return used + jnp.where(live, 1, 0)

        used = lax.fori_loop(0, half, place, 0)
        tbl_ref[2 * half + group] = (used + PER_TILE - 1) // PER_TILE
    tbl_ref[2 * half + 2] = first_ref[0]


def chunk_table(counts, chip, first, per_dev):
    smem = pl.BlockSpec(memory_space=pltpu.SMEM)
    return pl.pallas_call(
        functools.partial(chunk_table_body, per_dev),
        in_specs=[smem] * 3,
        out_specs=smem,
        out_shape=jax.ShapeDtypeStruct((2 * CHIPS * per_dev + 3,), jnp.int32),
        name='chunk_table',
    )(counts, chip, first)


def mlp_grad_body(sub, half, tbl_ref, *refs):
    nm_refs, low_refs, high_refs, far_refs = (refs[k * PER_TILE:(k + 1) * PER_TILE] for k in range(4))
    up_ref, down_ref, gup_ref, gdown_ref, nm_s, dt_s = refs[4 * PER_TILE:]
    tile = pl.program_id(1)
    fb = up_ref.shape[1]
    near = tbl_ref[2 * half]
    low = tbl_ref[2 * half + 2] == 1

    @pl.when(tile == 0)
    def _():
        gup_ref[...] = jnp.zeros_like(gup_ref)
        gdown_ref[...] = jnp.zeros_like(gdown_ref)

    def take(dst, srcs):
        for k in range(PER_TILE):
            dst[pl.ds(k * CHUNK, CHUNK), :] = srcs[k][...]

    @pl.when(tile < near + tbl_ref[2 * half + 1])
    def _():
        take(nm_s, nm_refs)

        @pl.when((tile < near) & low)
        def _():
            take(dt_s, low_refs)

        @pl.when((tile < near) & jnp.logical_not(low))
        def _():
            take(dt_s, high_refs)

        @pl.when(tile >= near)
        def _():
            take(dt_s, far_refs)

        for start in range(0, fb, sub):
            sl = pl.ds(start, sub)
            pre = dot(nm_s[...], up_ref[:, sl])
            d_act = dot(dt_s[...], down_ref[sl, :], NT)
            cdf = half_erf(pre)
            act = (pre * cdf).astype(BF)
            gdown_ref[sl, :] += dot(act, dt_s[...], TN)
            d_pre = (d_act * gelu_grad(pre, cdf)).astype(BF)
            gup_ref[:, sl] += dot(nm_s[...], d_pre, TN)


def mlp_grad(table, normed_all, near_low, near_high, far, w_up, w_down, fb=1280, sub=1280):
    tokens, dim = normed_all.shape
    ffn = w_up.shape[1]
    half = tokens // CHUNK // 2
    per_dev = half // CHIPS
    tiles = tokens // (CHUNK * PER_TILE)

    def group_chunk(entry):
        return entry // (2 * per_dev) * per_dev + entry % per_dev

    def any_spec(k):
        def index(f, t, tbl):
            near = tbl[2 * half]
            offset = jnp.where(t < near, t * PER_TILE, half + (jnp.minimum(t, near + tbl[2 * half + 1] - 1) - near) * PER_TILE)
            return tbl[offset + k], 0

        return pl.BlockSpec((CHUNK, dim), index)

    def near_spec(k, flag):
        def index(f, t, tbl):
            entry = group_chunk(tbl[jnp.minimum(t, tbl[2 * half] - 1) * PER_TILE + k])
            return jnp.where(tbl[2 * half + 2] == flag, entry, 0), 0

        return pl.BlockSpec((CHUNK, dim), index)

    def far_spec(k):
        def index(f, t, tbl):
            step = jnp.clip(t - tbl[2 * half], 0, tbl[2 * half + 1] - 1)
            return group_chunk(tbl[half + step * PER_TILE + k]), 0

        return pl.BlockSpec((CHUNK, dim), index)

    ks = range(PER_TILE)
    grid_spec = pltpu.PrefetchScalarGridSpec(
        num_scalar_prefetch=1,
        grid=(ffn // fb, tiles),
        in_specs=[any_spec(k) for k in ks] + [near_spec(k, 1) for k in ks] + [near_spec(k, 0) for k in ks] + [far_spec(k) for k in ks] + [
            pl.BlockSpec((dim, fb), lambda f, t, tbl: (0, f)),
            pl.BlockSpec((fb, dim), lambda f, t, tbl: (f, 0)),
        ],
        out_specs=[
            pl.BlockSpec((dim, fb), lambda f, t, tbl: (0, f)),
            pl.BlockSpec((fb, dim), lambda f, t, tbl: (f, 0)),
        ],
        scratch_shapes=[pltpu.VMEM((CHUNK * PER_TILE, dim), BF), pltpu.VMEM((CHUNK * PER_TILE, dim), BF)],
    )
    operands = [arr for arr in (normed_all, near_low, near_high, far) for _ in ks]
    return pl.pallas_call(
        functools.partial(mlp_grad_body, sub, half),
        grid_spec=grid_spec,
        out_shape=[jax.ShapeDtypeStruct((dim, ffn), F32), jax.ShapeDtypeStruct((ffn, dim), F32)],
        compiler_params=pltpu.CompilerParams(vmem_limit_bytes=62 * 1024 * 1024),
        cost_estimate=pl.CostEstimate(flops=8 * tokens * dim * ffn, bytes_accessed=12 * dim * ffn + 20 * tokens * dim, transcendentals=2 * tokens * ffn),
        name='mlp_grad',
    )(table, *operands, w_up, w_down)


def pair_mask(len_lo, len_hi):
    row = lax.broadcasted_iota(jnp.int32, (2 * SEQ, 2 * SEQ), 0)
    col = lax.broadcasted_iota(jnp.int32, (2 * SEQ, 2 * SEQ), 1)
    limit = jnp.where(row < SEQ, len_lo, len_hi + SEQ)
    floor = jnp.where(row < SEQ, 0, SEQ)
    return (col <= row) & (col < limit) & (col >= floor)


def head_masks():
    lane = lax.broadcasted_iota(jnp.int32, (1, 2 * HEAD), 1)
    low = jnp.where(lane < HEAD, 1.0, 0.0)
    return low.astype(BF), (1.0 - low).astype(BF)


def pair_softmax(query, key, visible):
    scores = jnp.where(visible, dot(query, key, NT) * HEAD ** -0.5, -1e30)
    weights = jnp.exp(scores - jnp.max(scores, axis=-1, keepdims=True))
    return weights * (1.0 / jnp.sum(weights, axis=-1, keepdims=True))


def attn_fwd_body(dim, len_ref, qkv_ref, ctx_ref):
    step = pl.program_id(0)
    visible = pair_mask(len_ref[2 * step], len_ref[2 * step + 1])
    masks = head_masks()
    for start in range(0, dim, 2 * HEAD):
        query = qkv_ref[:, pl.ds(start, 2 * HEAD)]
        key = qkv_ref[:, pl.ds(dim + start, 2 * HEAD)]
        value = qkv_ref[:, pl.ds(2 * dim + start, 2 * HEAD)]
        total = None
        for mask in masks:
            probs = pair_softmax(query * mask, key, visible).astype(BF)
            part = dot(probs, value * mask)
            total = part if total is None else total + part
        ctx_ref[:, pl.ds(start, 2 * HEAD)] = total.astype(BF)


def attn_fwd(lens, qkv):
    tokens, dim = qkv.shape[0], qkv.shape[1] // 3
    grid_spec = pltpu.PrefetchScalarGridSpec(
        num_scalar_prefetch=1,
        grid=(tokens // (2 * SEQ),),
        in_specs=[pl.BlockSpec((2 * SEQ, 3 * dim), lambda s, lens: (s, 0))],
        out_specs=pl.BlockSpec((2 * SEQ, dim), lambda s, lens: (s, 0)),
    )
    return pl.pallas_call(
        functools.partial(attn_fwd_body, dim),
        grid_spec=grid_spec,
        out_shape=jax.ShapeDtypeStruct((tokens, dim), BF),
        cost_estimate=pl.CostEstimate(flops=16 * tokens * 128 * dim, bytes_accessed=8 * tokens * dim, transcendentals=tokens * 128 * 20),
        name='attn_fwd',
    )(lens, qkv)


def attn_bwd_body(dim, len_ref, qkv_ref, dctx_ref, dqkv_ref):
    step = pl.program_id(0)
    visible = pair_mask(len_ref[2 * step], len_ref[2 * step + 1])
    masks = head_masks()
    for start in range(0, dim, 2 * HEAD):
        query = qkv_ref[:, pl.ds(start, 2 * HEAD)]
        key = qkv_ref[:, pl.ds(dim + start, 2 * HEAD)]
        value = qkv_ref[:, pl.ds(2 * dim + start, 2 * HEAD)]
        d_ctx = dctx_ref[:, pl.ds(start, 2 * HEAD)]
        d_query = d_key = d_value = 0.0
        for mask in masks:
            query_m, d_ctx_m = query * mask, d_ctx * mask
            probs = pair_softmax(query_m, key, visible)
            d_probs = dot(d_ctx_m, value, NT)
            inner = jnp.sum(probs * d_probs, axis=-1, keepdims=True)
            d_scores = (probs * (d_probs - inner) * HEAD ** -0.5).astype(BF)
            d_value = d_value + dot(probs.astype(BF), d_ctx_m, TN)
            d_query = d_query + dot(d_scores, key * mask)
            d_key = d_key + dot(d_scores, query_m, TN)
        dqkv_ref[:, pl.ds(start, 2 * HEAD)] = d_query.astype(BF)
        dqkv_ref[:, pl.ds(dim + start, 2 * HEAD)] = d_key.astype(BF)
        dqkv_ref[:, pl.ds(2 * dim + start, 2 * HEAD)] = d_value.astype(BF)


def attn_bwd(lens, qkv, d_ctx):
    tokens, dim = d_ctx.shape
    grid_spec = pltpu.PrefetchScalarGridSpec(
        num_scalar_prefetch=1,
        grid=(tokens // (2 * SEQ),),
        in_specs=[
            pl.BlockSpec((2 * SEQ, 3 * dim), lambda s, lens: (s, 0)),
            pl.BlockSpec((2 * SEQ, dim), lambda s, lens: (s, 0)),
        ],
        out_specs=pl.BlockSpec((2 * SEQ, 3 * dim), lambda s, lens: (s, 0)),
    )
    return pl.pallas_call(
        functools.partial(attn_bwd_body, dim),
        grid_spec=grid_spec,
        out_shape=jax.ShapeDtypeStruct((tokens, 3 * dim), BF),
        cost_estimate=pl.CostEstimate(flops=40 * tokens * 128 * dim, bytes_accessed=14 * tokens * dim, transcendentals=tokens * 128 * 20),
        name='attn_bwd',
    )(lens, qkv, d_ctx)


def solution(mesh):
    row_spec = P(('data', 'pipe'))
    stage_spec = P('pipe')
    swap = [(0, 1), (1, 0)]

    def flip_data(arr, bit):
        return lax.ppermute(arr, 'data', [(src, src ^ bit) for src in range(mesh.shape['data'])])

    def device_pass(acts_in, cot_out, seq_lens, w_qkv, w_out, w_up, w_down, gain_attn, gain_mlp):
        pipe = lax.axis_index('pipe')
        chip = lax.axis_index('data')
        seqs, seq, dim = acts_in.shape
        tokens = seqs * seq
        first = pipe == 0

        def gather_pair(part):
            return lax.all_gather(part, 'pipe', axis=0, tiled=True)

        wq = gather_pair(w_qkv)
        wo = gather_pair(w_out.reshape(1, dim, dim))
        mlp_weights = (w_up, w_down, lax.ppermute(w_up, 'pipe', swap), lax.ppermute(w_down, 'pipe', swap))
        owned = [(pipe == layer).astype(jnp.int32)[None] for layer in range(2)]
        gains_own = jnp.stack([gain_attn, gain_mlp], axis=1)
        gains_other = lax.ppermute(gains_own, 'pipe', swap)
        gains = jnp.where(first, jnp.concatenate([gains_own, gains_other]), jnp.concatenate([gains_other, gains_own])).astype(F32)

        pos = jnp.arange(seq)
        valid = pos[None, :] < seq_lens[:, None]
        cot = jnp.where(valid[:, :, None], cot_out, jnp.zeros_like(cot_out)).reshape(tokens, dim)

        order = jnp.arange(seqs)
        first_rank = jnp.sum(jnp.where(order[None, :] < order[:, None], seq_lens[None, :], 0), axis=1)
        rank = jnp.where(valid, first_rank[:, None] + pos[None, :], -1).reshape(1, tokens)
        pick = (rank == jnp.arange(tokens)[:, None]).astype(BF)

        count = jnp.full((8, 128), jnp.sum(seq_lens), jnp.int32)
        pair_counts = jnp.stack([count, lax.ppermute(count, 'pipe', swap)])
        half_counts = jnp.stack([pair_counts, flip_data(pair_counts, 1)])
        counts = jnp.concatenate([half_counts, flip_data(half_counts, 2)])[:, :, 0, 0].reshape(-1)
        table = chunk_table(counts, chip.astype(jnp.int32)[None], first.astype(jnp.int32)[None], tokens // CHUNK)

        cot_packed = dot(pick, cot_out.reshape(tokens, dim)).astype(BF)
        cot_group = lax.all_gather(cot_packed, 'data').reshape(-1, dim)

        saved = []
        hid = acts_in.reshape(tokens, dim)
        for layer in range(2):
            hid_f = hid.astype(F32)
            normed_a = norm_fwd(hid_f, gains[layer, 0])
            qkv = dot(normed_a, wq[layer]).astype(BF)
            ctx = attn_fwd(seq_lens, qkv)
            mid = (hid_f + dot(ctx, wo[layer])).astype(BF)
            normed_m = norm_fwd(mid.astype(F32), gains[layer, 1])
            out, pre = mlp_fwd(owned[layer], normed_m, mid, mlp_weights)
            saved.append((hid, normed_a, qkv, ctx, mid, normed_m, pre))
            hid = out
            if layer == 0:
                hid, table = lax.optimization_barrier((hid, table))
        acts_out = jnp.where(valid[:, :, None], hid.reshape(acts_in.shape), jnp.zeros_like(acts_in))

        def home(lower, upper):
            recv = lax.ppermute(jnp.where(first, upper, lower), 'pipe', swap)
            return jnp.where(first, lower, upper), recv

        nm_own = dot(pick, jnp.where(first, saved[0][5], saved[1][5])).astype(BF)
        nm_send = dot(pick, jnp.where(first, saved[1][5], saved[0][5])).astype(BF)
        nm_pair = jnp.stack([nm_own, lax.ppermute(nm_send, 'pipe', swap)])
        normed_all = lax.all_gather(nm_pair, 'data').reshape(-1, dim)
        na_home = home(saved[0][1], saved[1][1])
        ctx_home = home(saved[0][3], saved[1][3])

        d_hid = cot.astype(F32)
        d_mids, d_qkvs, d_gains = [None, None], [None, None], [None, None]
        for layer in (1, 0):
            hid_in, normed_a, qkv, ctx, mid, normed_m, pre = saved[layer]
            d_top = d_hid.astype(BF)
            if layer == 0:
                d_packed = dot(pick, d_top).astype(BF)
                d_group = lax.all_gather(d_packed, 'data').reshape(-1, dim)
            d_normed_m = mlp_bwd(owned[layer], d_top, pre, mlp_weights)
            d_norm, gain_m = norm_bwd(d_normed_m, mid.astype(F32), gains[layer, 1])
            d_mid = d_hid + d_norm
            d_mids[layer] = d_mid.astype(BF)
            d_ctx = dot(d_mids[layer], wo[layer], NT).astype(BF)
            d_qkvs[layer] = attn_bwd(seq_lens, qkv, d_ctx)
            d_normed_a = dot(d_qkvs[layer], wq[layer], NT)
            d_norm, gain_a = norm_bwd(d_normed_a, hid_in.astype(F32), gains[layer, 0])
            d_hid = d_mid + d_norm
            d_gains[layer] = jnp.stack([gain_a, gain_m])

        mid_home = home(*d_mids)
        qkv_home = home(*d_qkvs)
        g_qkv = dot(na_home[0], qkv_home[0], TN) + dot(na_home[1], qkv_home[1], TN)
        g_out = dot(ctx_home[0], mid_home[0], TN) + dot(ctx_home[1], mid_home[1], TN)

        d_group, g_qkv, g_out = lax.optimization_barrier((d_group, g_qkv, g_out))
        g_qkv, g_out = lax.psum((g_qkv, g_out), 'data')

        d_recv = lax.ppermute(jnp.where(first, cot_group, d_group), 'pipe', swap)
        grad_up, grad_down = mlp_grad(table, normed_all, d_group, cot_group, d_recv, w_up[0], w_down[0])

        gain_own, gain_recv = home(*d_gains)
        g_gain = gain_own + gain_recv
        g_gain = g_gain + flip_data(g_gain, 1)
        g_gain = g_gain + flip_data(g_gain, 2)
        return (acts_out, g_qkv[None], g_out.reshape(w_out.shape), grad_up[None], grad_down[None], g_gain[:1], g_gain[1:])

    return jax.shard_map(device_pass, mesh=mesh, in_specs=(row_spec, row_spec, row_spec) + (stage_spec,) * 6, out_specs=(row_spec,) + (stage_spec,) * 6, check_vma=False)
```
